32 devices in a mesh: lat: 4 (over y, core), lon: 8 (over z, x).
Axes of the slice: x: 2, y: 2, z: 4, core: 2. Of those that a mesh axis runs over, the one named last changes fastest.
Arguments:
- forcing: float32 [640, 1024], P('lat', 'lon'), may hold values from -28 to 28
- search_direction: float32 [640, 1024], P('lat', 'lon'), may hold values from -28 to 28
- ocean_depth: float32 [640, 1024], P('lat', 'lon'), may hold values from 0.5 to 8
- land_mask: int32 [640, 1024], P('lat', 'lon'), may hold values 0 or 1
- fold_map: int32 [1024], replicated, may hold values from 0 to 1023, as said below
Outputs:
- scaled_height: float32 [640, 1024], P('lat', 'lon')
- residual: float32 [640, 1024], P('lat', 'lon')
The draws below stay inside these ranges and needn't reach their ends.
Inputs may be any that keep to these rules, and one draw needn't show every extreme that they name: `fold_map`: column j's partner across the fold is (c - j) mod 1024 for one c of 0 to 1023, so the map is its own inverse.
All inputs are finite; a program needn't handle non-finite values. No bound on the sum of `land_mask` on one device may be relied on, other than what follows from the above.
Results may differ from the reference program's by a relative error of at most 0.0003.
Values sent between devices are 32-bit elements; how exact they have to be, the bound alone decides.
A program may use at most 64 MiB of HBM per device.

```python
import math
import jax
import jax.numpy as jnp
import numpy as np
from jax import lax

STEPS = 8
OUTER = 1
REACH = 256
NX = 640
NY = 1024


def field_profile():
    lat_ramp = jnp.arange(NX, dtype=jnp.float32) / NX
    lon_ramp = jnp.arange(NY, dtype=jnp.float32) / NY
    north_gap = (NX - 1 - jnp.arange(NX, dtype=jnp.float32)) / 8.0
    north_boost = 1.0 + 1.5 * jnp.exp(-north_gap)
    return jnp.exp(jnp.log(3.0) * (lat_ramp[:, None] + lon_ramp[None, :])) * north_boost[:, None]


def rough_field(key):
    first_key = jax.random.fold_in(key, 0)
    values = jax.random.truncated_normal(first_key, -4.0, 4.0, (NX, NY), jnp.float32)
    return (0.3 * values * field_profile()).astype(jnp.float32)


def draw_forcing(key, part):
    return rough_field(jax.random.fold_in(key, 11))


def draw_search_direction(key, part):
    return rough_field(jax.random.fold_in(key, 23))


def draw_fold_map(key, part):
    pivot_column = jax.random.randint(jax.random.fold_in(key, 7), (), 0, NY, dtype=jnp.int32)
    return ((pivot_column - jnp.arange(NY, dtype=jnp.int32)) % NY).astype(jnp.int32)


def set_ends(drawn, stream_key, smallest, top_value):
    longest = drawn.shape.index(max(drawn.shape))
    spots = []
    for shift in (0, 1):
        where = [jax.random.randint(jax.random.fold_in(stream_key, axis), (), 0, length) for axis, length in enumerate(drawn.shape)]
        where[longest] = (where[longest] + shift) % drawn.shape[longest]
        spots.append(tuple(where))
    return drawn.at[spots[0]].set(smallest).at[spots[1]].set(top_value)


def level_of(key, extent, pieces, low, largest):
    level = 1.0
    for dim, shards_of in pieces:
        draws = jax.random.uniform(jax.random.fold_in(jax.random.fold_in(key, 6), dim), (shards_of,), jnp.float32, low / len(pieces), largest / len(pieces))
        level = level * jnp.repeat(jnp.exp(draws), extent[dim] // shards_of).reshape((-1,) + (1,) * (len(extent) - 1 - dim))
    return level


def setup_inputs(seed: int = 0) -> dict:
    key_of = jax.random.split(jax.random.key(seed), 6)
    forcing = draw_forcing(jax.random.fold_in(key_of[5], 71), 0)
    search_direction = draw_search_direction(jax.random.fold_in(key_of[5], 71), 0)
    ocean_depth = jnp.clip(jnp.exp(math.log(8.0) - 2.7725887 * jax.random.uniform(key_of[2], (NX, NY), jnp.float32) ** level_of(key_of[2], (NX, NY), ((0, 4), (1, 8)), -0.2, 0.2)), 0.5, 8.0)
    land_mask = set_ends((jax.random.randint(key_of[3], (NX, NY), 0, 8) < 7).astype(jnp.int32), jax.random.fold_in(key_of[3], 1), 0, 1)
    fold_map = draw_fold_map(jax.random.fold_in(key_of[5], 71), 0)
    return dict(forcing=forcing, search_direction=search_direction, ocean_depth=ocean_depth, land_mask=land_mask, fold_map=fold_map)


PRECISE = lax.Precision.HIGHEST
DIRECTIONS = ((1, 0), (-1, 0), (0, 1), (0, -1), (1, 1), (-1, -1), (1, -1), (-1, 1))
LINK_FACTORS = (1.0, 1.0, 1.0, 1.0, 0.5, 0.5, 0.5, 0.5)

def chebyshev_table(basis_steps):
    number = 2 * basis_steps + 1
    matrix = np.zeros((number, number), np.float32)
    for offset, length in ((0, basis_steps + 1), (basis_steps + 1, basis_steps)):
        for column in range(length - 1):
            matrix[offset + column, offset + column] = 1.0
            if column == 0:
                matrix[offset + 1, offset] = 1.0
            else:
                matrix[offset + column + 1, offset + column] = 0.5
                matrix[offset + column - 1, offset + column] = 0.5
    return matrix

def coordinates(gram_matrix, basis_steps):
    number = 2 * basis_steps + 1
    shift_matrix = jnp.asarray(chebyshev_table(basis_steps))
    unit_rows = jnp.eye(number, dtype=jnp.float32)
    solution_coords = jnp.zeros((number,), jnp.float32)
    direction_coords = unit_rows[0]
    residual_coords = unit_rows[basis_steps + 1]
    norm_now = jnp.dot(residual_coords, jnp.dot(gram_matrix, residual_coords, precision=PRECISE), precision=PRECISE)
    for inner_step in range(basis_steps):
        mapped = jnp.dot(shift_matrix, direction_coords, precision=PRECISE)
        curvature = jnp.dot(direction_coords, jnp.dot(gram_matrix, mapped, precision=PRECISE), precision=PRECISE)
        step_length = norm_now / curvature
        solution_coords = solution_coords + step_length * direction_coords
        residual_coords = residual_coords - step_length * mapped
        norm_next = jnp.dot(residual_coords, jnp.dot(gram_matrix, residual_coords, precision=PRECISE), precision=PRECISE)
        direction_coords = residual_coords + norm_next / norm_now * direction_coords
        norm_now = norm_next
    return (solution_coords, residual_coords, direction_coords)

def pad_ghosts(source, fold_map):
    fold_row = jnp.take(source[-1], fold_map)
    zeros_row = jnp.zeros((1, source.shape[1]), source.dtype)
    stacked = jnp.concatenate([zeros_row, source, fold_row[None, :]], axis=0)
    return jnp.concatenate([stacked[:, -1:], stacked, stacked[:, :1]], axis=1)

def neighbour(padded, north_step, east_step):
    row_total = padded.shape[0] - 2
    column_total = padded.shape[1] - 2
    return padded[1 + north_step:1 + north_step + row_total, 1 + east_step:1 + east_step + column_total]

def reference(forcing, search_direction, ocean_depth, land_mask, fold_map):
    ocean_flag = land_mask.astype(jnp.float32)
    column_depth = ocean_depth * ocean_flag
    padded_depth = pad_ghosts(column_depth, fold_map)
    padded_wet = (padded_depth > 0.0).astype(jnp.float32)
    centre_wet = padded_wet[1:-1, 1:-1]
    weight_list = []
    link_sum = jnp.zeros_like(column_depth)
    for direction_index in range(8):
        north_step, east_step = DIRECTIONS[direction_index]
        weight = LINK_FACTORS[direction_index] * 0.5 * (column_depth + neighbour(padded_depth, north_step, east_step)) * centre_wet * neighbour(padded_wet, north_step, east_step)
        weight_list.append(weight)
        link_sum = link_sum + weight
    diagonal = centre_wet * (column_depth / (REACH * REACH) + link_sum) + (1.0 - centre_wet)
    inverse_root = lax.rsqrt(diagonal)

    def operate(source):
        padded = pad_ghosts(inverse_root * source, fold_map)
        running = jnp.zeros_like(source)
        for direction_index in range(8):
            north_step, east_step = DIRECTIONS[direction_index]
            running = running + weight_list[direction_index] * neighbour(padded, north_step, east_step)
        return -inverse_root * running
    operate_many = jax.vmap(operate)
    scaled_height = jnp.zeros_like(forcing)
    residual = ocean_flag * forcing
    direction = ocean_flag * search_direction
    for outer_step in range(OUTER):
        earlier = jnp.stack([direction, residual])
        current = operate_many(earlier)
        stored = [earlier, current]
        for power in range(1, STEPS):
            if power == STEPS - 1:
                earlier = earlier[:1]
                current = current[:1]
            upcoming = 2.0 * operate_many(current) - earlier
            earlier = current
            current = upcoming
            stored.append(current)
        krylov_basis = jnp.stack([member[0] for member in stored] + [member[1] for member in stored[:STEPS]])
        flattened = krylov_basis.reshape(krylov_basis.shape[0], -1)
        gram_matrix = jnp.dot(flattened, flattened.T, precision=PRECISE)
        solution_coords, residual_coords, direction_coords = coordinates(gram_matrix, STEPS)
        scaled_height = scaled_height + jnp.einsum('k,kij->ij', solution_coords, krylov_basis, precision=PRECISE)
        residual = jnp.einsum('k,kij->ij', residual_coords, krylov_basis, precision=PRECISE)
        direction = jnp.einsum('k,kij->ij', direction_coords, krylov_basis, precision=PRECISE)
    return (scaled_height, residual)
```

```python
import functools

import jax
import jax.numpy as jnp
from jax import lax
from jax.experimental import pallas as pl
from jax.experimental.pallas import tpu as pltpu
from jax.sharding import PartitionSpec as P

STEPS = 8
REACH = 256
MESH = pl.DeviceIdType.MESH
PAD = 16
GROUP = 32
CHUNK = 16

DIRECTIONS = ((1, 0), (-1, 0), (0, 1), (0, -1), (1, 1), (-1, -1), (1, -1), (-1, 1))
SLOT = {offset: index for index, offset in enumerate(DIRECTIONS)}


def halves(offset):
    return 0.5 if 0 in offset else 0.25


def chunks_of(low, high, size):
    return [(at, min(size, high - at)) for at in range(low, high, size)]


def shift_pair(centre, halo, step):
    width = centre.shape[1]
    lane = lax.broadcasted_iota(jnp.int32, centre.shape, 1)
    edge = lane == (0 if step == 1 else width - 1)
    turn = width - 1 if step == 1 else 1
    return (
        pltpu.roll(jnp.where(edge, halo, centre), turn, 1),
        pltpu.roll(jnp.where(edge, centre, halo), turn, 1),
    )


def turned(x, shift):
    shift = shift % x.shape[1]
    return x if shift == 0 else pltpu.roll(x, shift, 1)


def bilinear(left, right, gram):
    total = None
    for i in sorted(left):
        inner = None
        for j in sorted(right):
            term = gram(i, j) * right[j]
            inner = term if inner is None else inner + term
        inner = left[i] * inner
        total = inner if total is None else total + inner
    return total


def plus(left, right):
    result = dict(left)
    for key, value in right.items():
        result[key] = result[key] + value if key in result else value
    return result


def scaled(factor, vector):
    return {key: factor * value for key, value in vector.items()}


def apply_shift(vector):
    result = {}
    for (chain, power), value in vector.items():
        parts = [((chain, power), value)]
        if power == 0:
            parts.append(((chain, 1), value))
        else:
            half = 0.5 * value
            parts += [((chain, power + 1), half), ((chain, power - 1), half)]
        result = plus(result, {}) if not parts else result
        for key, part in parts:
            result = plus(result, {key: part})
    return result


def coordinates(moments):
    cache = {}

    def gram(left, right):
        kind = (left[0], right[0]) if left[0] <= right[0] else (right[0], left[0])
        low, high = sorted((left[1], right[1]))
        key = (kind, low, high)
        if key not in cache:
            series = moments[kind]
            cache[key] = 0.5 * (series[high + low] + series[high - low])
        return cache[key]

    solution_coords = {}
    one = jnp.ones_like(moments[("p", "p")][0])
    direction_coords = {("p", 0): one}
    residual_coords = {("r", 0): one}
    norm_now = bilinear(residual_coords, residual_coords, gram)
    for _ in range(STEPS):
        mapped = apply_shift(direction_coords)
        step_length = norm_now / bilinear(direction_coords, mapped, gram)
        solution_coords = plus(solution_coords, scaled(step_length, direction_coords))
        residual_coords = plus(residual_coords, scaled(-step_length, mapped))
        norm_next = bilinear(residual_coords, residual_coords, gram)
        direction_coords = plus(
            residual_coords, scaled(norm_next / norm_now, direction_coords)
        )
        norm_now = norm_next
    return solution_coords, residual_coords


def fold_sublanes(parts):
    row = lax.broadcasted_iota(jnp.int32, parts[0].shape, 0)
    parts = list(parts)
    span = 4
    while span:
        low = (row & span) == 0
        half = len(parts) // 2
        parts = [
            jnp.where(low, first, second)
            + pltpu.roll(jnp.where(low, second, first), span, 0)
            if span == 4
            else jnp.where(low, first, second)
            + jnp.where(low, pltpu.roll(first, 8 - span, 0), pltpu.roll(second, span, 0))
            for first, second in zip(parts[:half], parts[half:])
        ]
        span //= 2
    return parts[0]


def kernel(
    n_lat, n_lon, forcing, search, depth_in, mask_in, fold_map, out_height, out_residual,
    depth, depth_e, depth_w, root, root_e, root_w, weights, basis, basis_halo,
    row_north, row_south, fold_rows, packed, got_north, got_south, got_east, got_west,
    corners, fold_all, dots, sums_lat, sums_lon, moment_rows,
    near_send, near_recv, fold_send, fold_recv, lat_send, lat_recv, lon_send, lon_recv,
):
    rows, width = forcing.shape
    lat, lon = lax.axis_index("lat"), lax.axis_index("lon")
    top = n_lat - 1
    north, south = lax.rem(lat + 1, n_lat), lax.rem(lat + n_lat - 1, n_lat)
    east, west = lax.rem(lon + 1, n_lon), lax.rem(lon + n_lon - 1, n_lon)
    has_north, has_south = lat < top, lat > 0
    group_rows = rows * GROUP // width
    n_groups = width // GROUP

    barrier = pltpu.get_barrier_semaphore()

    def greet(place):
        pl.semaphore_signal(barrier, inc=1, device_id=place, device_id_type=MESH)

    for d in range(1, n_lat):
        greet((lax.rem(lat + d, n_lat), lon))
    for d in range(1, n_lon):
        greet((lat, lax.rem(lon + d, n_lon)))

    for place in ((north, east), (north, west), (south, east), (south, west)):
        greet(place)

    lane_group = lax.broadcasted_iota(jnp.int32, (group_rows, width), 1)
    west_edge = east_edge = None
    for g in range(n_groups):
        here = pl.ds(g * group_rows, group_rows)
        there = pl.ds(PAD + g * group_rows, group_rows)
        flag = mask_in[here, :].astype(jnp.float32)
        deep = depth_in[here, :] * flag
        moving = search[here, :] * flag
        left = forcing[here, :] * flag
        depth[0, there, :] = deep
        basis[0, there, :] = moving
        basis[STEPS + 1, there, :] = left
        inside = lane_group - g * GROUP
        to_west = jnp.where(
            inside < 9,
            turned(deep, g * GROUP),
            jnp.where(inside < 17, turned(moving, g * GROUP + 9), turned(left, g * GROUP + 17)),
        )
        to_east = jnp.where(
            inside < 9,
            turned(deep, g * GROUP + 9),
            jnp.where(inside < 17, turned(moving, g * GROUP + 17), turned(left, g * GROUP + 25)),
        )
        west_edge = to_west if g == 0 else jnp.where(inside >= 0, to_west, west_edge)
        east_edge = to_east if g == 0 else jnp.where(inside >= 0, to_east, east_edge)
    packed[0] = west_edge
    packed[1] = east_edge
    first, last = PAD, PAD + rows
    row_south[0:16, :] = depth[0, first : first + 16, :]
    row_south[16:24, :] = basis[0, first : first + 8, :]
    row_south[24:32, :] = basis[STEPS + 1, first : first + 8, :]
    row_north[0:16, :] = depth[0, last - 16 : last, :]
    row_north[16:24, :] = basis[0, last - 8 : last, :]
    row_north[24:32, :] = basis[STEPS + 1, last - 8 : last, :]

    @pl.when(lat == top)
    def _():
        for r in range(16):
            fold_rows[r : r + 1, :] = depth[0, last - 1 - r : last - r, :]
        for r in range(8):
            fold_rows[16 + r : 17 + r, :] = basis[0, last - 1 - r : last - r, :]
            fold_rows[24 + r : 25 + r, :] = basis[STEPS + 1, last - 1 - r : last - r, :]
        fold_all[lon] = fold_rows[...]

    pl.semaphore_wait(barrier, n_lat - 1 + n_lon - 1 + 4)

    def near(index, source, target, place):
        return pltpu.make_async_remote_copy(
            src_ref=source, dst_ref=target, send_sem=near_send.at[index],
            recv_sem=near_recv.at[index], device_id=place, device_id_type=MESH,
        )

    tail = pl.ds(group_rows - 16, 16)
    head = pl.ds(0, 16)
    to_north = near(0, row_north, got_south, (north, lon))
    to_south = near(1, row_south, got_north, (south, lon))
    to_east = near(2, packed.at[1], got_west, (lat, east))
    to_west = near(3, packed.at[0], got_east, (lat, west))
    to_ne = near(4, packed.at[1, tail], corners.at[0], (north, east))
    to_nw = near(5, packed.at[0, tail], corners.at[1], (north, west))
    to_se = near(6, packed.at[1, head], corners.at[2], (south, east))
    to_sw = near(7, packed.at[0, head], corners.at[3], (south, west))
    northward, southward = (to_north, to_ne, to_nw), (to_south, to_se, to_sw)

    def spread(source, slots, send_sem, recv_sem, along_lat):
        size = n_lat if along_lat else n_lon
        me = lat if along_lat else lon
        copies = []
        for d in range(1, size):
            peer = lax.rem(me + d, size)
            copies.append(
                pltpu.make_async_remote_copy(
                    src_ref=source, dst_ref=slots.at[me], send_sem=send_sem.at[d - 1],
                    recv_sem=recv_sem.at[d - 1],
                    device_id=(peer, lon) if along_lat else (lat, peer),
                    device_id_type=MESH,
                )
            )
        return copies

    across = spread(fold_rows, fold_all, fold_send, fold_recv, False)

    @pl.when(lat == top)
    def _():
        for copy in across:
            copy.start()

    to_east.start()
    to_west.start()

    @pl.when(has_north)
    def _():
        for copy in northward:
            copy.start()

    @pl.when(has_south)
    def _():
        for copy in southward:
            copy.start()

    def unpack(got_e, got_w, start, g, count):
        lane = lax.broadcasted_iota(jnp.int32, (count, width), 1)
        base = -g * GROUP
        spans = ((0, 9, depth.at[1]), (9, 8, basis_halo.at[0]), (17, 8, basis_halo.at[STEPS + 1]))
        for offset, cells, target in spans:
            from_east = turned(got_e, base - offset)
            from_west = turned(got_w, base - offset - cells)
            target[start : start + count, :] = jnp.where(
                lane < cells,
                from_east,
                jnp.where(lane >= width - cells, from_west, jnp.zeros_like(got_e)),
            )

    to_east.wait_recv()
    to_west.wait_recv()
    for g in range(n_groups):
        unpack(got_east[...], got_west[...], PAD + g * group_rows, g, group_rows)

    @pl.when(has_south)
    def _():
        for copy in northward:
            copy.wait_recv()
        depth[0, 0:16, :] = got_south[0:16, :]
        basis[0, 8:16, :] = got_south[16:24, :]
        basis[STEPS + 1, 8:16, :] = got_south[24:32, :]
        unpack(corners[1], corners[0], 0, n_groups - 1, 16)

    @pl.when(lat == 0)
    def _():
        nothing = jnp.zeros((16, width), jnp.float32)
        for target in (depth.at[0], depth.at[1]):
            target[0:16, :] = nothing
        for power in (0, STEPS + 1):
            basis[power, 0:16, :] = nothing
            basis_halo[power, 0:16, :] = nothing

    @pl.when(has_north)
    def _():
        for copy in southward:
            copy.wait_recv()
        depth[0, last : last + 16, :] = got_north[0:16, :]
        basis[0, last : last + 8, :] = got_north[16:24, :]
        basis[STEPS + 1, last : last + 8, :] = got_north[24:32, :]
        unpack(corners[3], corners[2], last, 0, 16)

    @pl.when(lat == top)
    def _():
        for copy in across:
            copy.wait_recv()
        total = n_lon * width
        pivot = lax.rem(fold_map[0] - lon * width + total, total)
        block, offset = pivot // width, lax.rem(pivot, width)
        lane = lax.broadcasted_iota(jnp.int32, (32, width), 1)
        index = lax.rem(offset - lane + width, width)

        def mirrored(which):
            rows_of = fold_all[lax.rem(block + which + n_lon, n_lon)]
            return jnp.take_along_axis(rows_of, index, axis=1, mode="promise_in_bounds")

        ahead, same, behind, beyond = (mirrored(which) for which in (1, 0, -1, -2))
        close = lane <= offset
        centre = jnp.where(close, same, behind)
        halo = jnp.where(
            lane < width // 2, jnp.where(close, behind, beyond), jnp.where(close, ahead, same)
        )
        for value, deep, fields in ((centre, depth.at[0], basis), (halo, depth.at[1], basis_halo)):
            deep[last : last + 16, :] = value[0:16, :]
            fields[0, last : last + 8, :] = value[16:24, :]
            fields[STEPS + 1, last : last + 8, :] = value[24:32, :]

    low, high = PAD - 8, last + 8
    for at, count in chunks_of(0, rows + 2 * PAD, CHUNK):
        span = pl.ds(at, count)
        centre, halo = depth[0, span, :], depth[1, span, :]
        depth_e[0, span, :], depth_e[1, span, :] = shift_pair(centre, halo, 1)
        depth_w[0, span, :], depth_w[1, span, :] = shift_pair(centre, halo, -1)
    shifted_depth = {0: depth, 1: depth_e, -1: depth_w}
    for at, count in chunks_of(low, high, CHUNK):
        roots = []
        for tile in (0, 1):
            here = depth[tile, at : at + count, :]
            sums = {0.5: None, 0.25: None}
            for a, b in DIRECTIONS:
                beside = shifted_depth[b][tile, at + a : at + a + count, :]
                link = jnp.where(beside > 0.0, here + beside, 0.0)
                factor = halves((a, b))
                sums[factor] = link if sums[factor] is None else sums[factor] + link
            diagonal = here * (1.0 / (REACH * REACH)) + (0.5 * sums[0.5] + 0.25 * sums[0.25])
            value = lax.rsqrt(jnp.where(here > 0.0, diagonal, 1.0))
            root[tile, at : at + count, :] = value
            roots.append(value)
        span = pl.ds(at, count)
        root_e[0, span, :], root_e[1, span, :] = shift_pair(roots[0], roots[1], 1)
        root_w[0, span, :], root_w[1, span, :] = shift_pair(roots[0], roots[1], -1)
    shifted_root = {0: root, 1: root_e, -1: root_w}
    for at, count in chunks_of(low, high, CHUNK):
        for tile in (0, 1):
            for b in (-1, 0, 1):
                goal_depth = shifted_depth[-b][tile, at : at + count, :]
                goal_root = shifted_root[-b][tile, at : at + count, :]
                goal_wet = goal_depth > 0.0
                for a in (-1, 0, 1):
                    if (a, b) == (0, 0):
                        continue
                    from_depth = depth[tile, at + a : at + a + count, :]
                    from_root = root[tile, at + a : at + a + count, :]
                    link = jnp.where(
                        jnp.minimum(goal_depth, from_depth) > 0.0, goal_depth + from_depth, 0.0
                    )
                    weights[SLOT[(a, b)], tile, at : at + count, :] = (
                        goal_root * (-2.0 * halves((a, b)))
                    ) * (link * from_root)

    dot_sums = {}

    def add_dot(key, left, right):
        product = left * right
        for r in range(0, product.shape[0], 8):
            piece = product[r : r + 8, :]
            dot_sums[key] = piece if key not in dot_sums else dot_sums[key] + piece

    row_chunks = [(low, 8)] + chunks_of(first, last, CHUNK) + [(last, 8)]
    for at, count in chunks_of(first, last, CHUNK):
        p0 = basis[0, at : at + count, :]
        r0 = basis[STEPS + 1, at : at + count, :]
        add_dot(("p", "p", 0), p0, p0)
        add_dot(("r", "r", 0), r0, r0)
        add_dot(("p", "r", 0), p0, r0)

    for power in range(1, STEPS + 1):
        chains = [("p", 0, power == STEPS)]
        if power < STEPS:
            chains.append(("r", STEPS + 1, power == STEPS - 1))
        for at, count in row_chunks:
            inner = first <= at < last
            fresh = {}
            held = {}
            factors = [
                {ab: weights[SLOT[ab], tile, at : at + count, :] for ab in DIRECTIONS}
                for tile in (0, 1)
            ]
            for name, origin, only_block in chains:
                if only_block and not inner:
                    continue
                slot = origin + power
                parts = []
                for tile, fields in ((0, basis), (1, basis_halo)):
                    taken = {
                        a: fields[slot - 1, at + a : at + a + count, :] for a in (-1, 0, 1)
                    }
                    if tile == 0:
                        held[name] = taken[0]
                    columns = {}
                    for b in (-1, 0, 1):
                        total = None
                        for a in (-1, 0, 1):
                            if (a, b) == (0, 0):
                                continue
                            term = factors[tile][(a, b)] * taken[a]
                            total = term if total is None else total + term
                        columns[b] = total
                    parts.append(columns)
                ahead = shift_pair(parts[0][1], parts[1][1], 1)
                behind = shift_pair(parts[0][-1], parts[1][-1], -1)
                for tile, fields in ((0, basis), (1, basis_halo)):
                    if tile == 1 and only_block:
                        continue
                    value = parts[tile][0] + ahead[tile] + behind[tile]
                    if power == 1:
                        value = 0.5 * value
                    else:
                        value = value - fields[slot - 2, at : at + count, :]
                    fields[slot, at : at + count, :] = value
                    if tile == 0:
                        fresh[name] = value
            if not inner:
                continue
            for name, _, _ in chains:
                add_dot((name, name, 2 * power), fresh[name], fresh[name])
                add_dot((name, name, 2 * power - 1), fresh[name], held[name])
            if power < STEPS:
                add_dot(("p", "r", 2 * power), fresh["p"], fresh["r"])
                add_dot(("p", "r", 2 * power - 1), fresh["p"], held["r"])
            else:
                add_dot(
                    ("p", "r", 2 * power - 1),
                    fresh["p"],
                    basis[STEPS + power, at : at + count, :],
                )
        for key in [key for key in dot_sums]:
            dots[order_of()[key]] = dot_sums.pop(key)

    number = len(order_of())
    lane = lax.broadcasted_iota(jnp.int32, (8, width), 1)
    message = jnp.zeros((8, width), jnp.float32)
    for g in range(number // 8):
        grouped = fold_sublanes([dots[8 * g + s] for s in range(8)])
        message = jnp.where(lane == g, jnp.sum(grouped, axis=1, keepdims=True), message)
    for slots, size, along_lat, send_sem, recv_sem in (
        (sums_lat, n_lat, True, lat_send, lat_recv),
        (sums_lon, n_lon, False, lon_send, lon_recv),
    ):
        me = lat if along_lat else lon
        slots[me] = message
        copies = spread(slots.at[me], slots, send_sem, recv_sem, along_lat)
        for copy in copies:
            copy.start()
        for copy in copies:
            copy.wait_recv()
        message = slots[0]
        for index in range(1, size):
            message = message + slots[index]
        for copy in copies:
            copy.wait_send()
    for g in range(number // 8):
        picked = jnp.sum(jnp.where(lane == g, message, 0.0), axis=1, keepdims=True)
        moment_rows[8 * g : 8 * g + 8, :] = jnp.broadcast_to(picked, (8, width))
    moments = {}
    for kind in (("p", "p"), ("p", "r"), ("r", "r")):
        series = []
        for index in range(17 if kind == ("p", "p") else 16 if kind == ("p", "r") else 15):
            spot = order_of()[kind + (index,)]
            value = jnp.broadcast_to(moment_rows[spot : spot + 1, :], (8, width))
            series.append(value if index < 2 else 2.0 * value - series[index % 2])
        moments[kind] = series
    height_coords, residual_coords = coordinates(moments)
    for at in range(0, rows, 8):
        for coords, out in ((height_coords, out_height), (residual_coords, out_residual)):
            total = None
            for (chain, power), factor in sorted(coords.items(), key=lambda item: item[0]):
                slot = power + (0 if chain == "p" else STEPS + 1)
                term = factor * basis[slot, PAD + at : PAD + at + 8, :]
                total = term if total is None else total + term
            out[at : at + 8, :] = total

    to_east.wait_send()
    to_west.wait_send()

    @pl.when(has_north)
    def _():
        for copy in northward:
            copy.wait_send()

    @pl.when(has_south)
    def _():
        for copy in southward:
            copy.wait_send()

    @pl.when(lat == top)
    def _():
        for copy in across:
            copy.wait_send()


@functools.cache
def order_of():
    keys = [("p", "p", k) for k in range(2 * STEPS + 1)]
    keys += [("p", "r", k) for k in range(2 * STEPS)]
    keys += [("r", "r", k) for k in range(2 * STEPS - 1)]
    return {key: index for index, key in enumerate(keys)}


def per_device(n_lat, n_lon, forcing, search_direction, ocean_depth, land_mask, fold_map):
    rows, width = forcing.shape
    tall = rows + 2 * PAD
    f32 = jnp.float32
    pair = pltpu.VMEM((2, tall, width), f32)
    edge = pltpu.VMEM((32, width), f32)
    group_rows = rows * GROUP // width
    strip = pltpu.VMEM((group_rows, width), f32)
    dma = pltpu.SemaphoreType.DMA
    block = pl.BlockSpec(memory_space=pltpu.VMEM)
    return pl.pallas_call(
        functools.partial(kernel, n_lat, n_lon),
        out_shape=[jax.ShapeDtypeStruct((rows, width), f32)] * 2,
        in_specs=[block] * 4 + [pl.BlockSpec(memory_space=pltpu.SMEM)],
        out_specs=[block] * 2,
        scratch_shapes=[
            pair, pair, pair, pair, pair, pair,
            pltpu.VMEM((8, 2, tall, width), f32),
            pltpu.VMEM((2 * STEPS + 1, tall, width), f32),
            pltpu.VMEM((2 * STEPS + 1, tall, width), f32),
            edge, edge, edge,
            pltpu.VMEM((2, group_rows, width), f32),
            edge, edge, strip, strip,
            pltpu.VMEM((4, 16, width), f32),
            pltpu.VMEM((n_lon, 32, width), f32),
            pltpu.VMEM((6 * STEPS, 8, width), f32),
            pltpu.VMEM((n_lat, 8, width), f32),
            pltpu.VMEM((n_lon, 8, width), f32),
            pltpu.VMEM((6 * STEPS, width), f32),
            dma((8,)), dma((8,)),
            dma((n_lon - 1,)), dma((n_lon - 1,)),
            dma((n_lat - 1,)), dma((n_lat - 1,)),
            dma((n_lon - 1,)), dma((n_lon - 1,)),
        ],
        compiler_params=pltpu.CompilerParams(collective_id=0, has_side_effects=True),
        name="tripole_cg",
    )(forcing, search_direction, ocean_depth, land_mask, fold_map)


def solution(mesh):
    cells = P("lat", "lon")
    return jax.shard_map(
        functools.partial(per_device, mesh.shape["lat"], mesh.shape["lon"]),
        mesh=mesh,
        in_specs=(cells, cells, cells, cells, P()),
        out_specs=(cells, cells),
        check_vma=False,
    )
```

```python
import functools

import jax
import jax.numpy as jnp
from jax import lax
from jax.experimental import pallas as pl
from jax.experimental.pallas import tpu as pltpu
from jax.sharding import PartitionSpec as P

STEPS = 8
REACH = 256
MESH = pl.DeviceIdType.MESH
PAD = 16
GROUP = 32
CHUNK = 16
DIRECT_LIMIT = 64

DIRECTIONS = ((1, 0), (-1, 0), (0, 1), (0, -1), (1, 1), (-1, -1), (1, -1), (-1, 1))
SLOT = {offset: index for index, offset in enumerate(DIRECTIONS)}


def halves(offset):
    return 0.5 if 0 in offset else 0.25


def chunks_of(low, high, size):
    return [(at, min(size, high - at)) for at in range(low, high, size)]


def shift_pair(centre, halo, step):
    width = centre.shape[1]
    lane = lax.broadcasted_iota(jnp.int32, centre.shape, 1)
    edge = lane == (0 if step == 1 else width - 1)
    turn = width - 1 if step == 1 else 1
    return (
        pltpu.roll(jnp.where(edge, halo, centre), turn, 1),
        pltpu.roll(jnp.where(edge, centre, halo), turn, 1),
    )


def turned(x, shift):
    shift = shift % x.shape[1]
    return x if shift == 0 else pltpu.roll(x, shift, 1)


def bilinear(left, right, gram):
    total = None
    for i in sorted(left):
        inner = None
        for j in sorted(right):
            term = gram(i, j) * right[j]
            inner = term if inner is None else inner + term
        inner = left[i] * inner
        total = inner if total is None else total + inner
    return total


def plus(left, right):
    result = dict(left)
    for key, value in right.items():
        result[key] = result[key] + value if key in result else value
    return result


def scaled(factor, vector):
    return {key: factor * value for key, value in vector.items()}


def apply_shift(vector):
    result = {}
    for (chain, power), value in vector.items():
        parts = [((chain, power), value)]
        if power == 0:
            parts.append(((chain, 1), value))
        else:
            half = 0.5 * value
            parts += [((chain, power + 1), half), ((chain, power - 1), half)]
        result = plus(result, {}) if not parts else result
        for key, part in parts:
            result = plus(result, {key: part})
    return result


def coordinates(moments):
    cache = {}

    def gram(left, right):
        kind = (left[0], right[0]) if left[0] <= right[0] else (right[0], left[0])
        low, high = sorted((left[1], right[1]))
        key = (kind, low, high)
        if key not in cache:
            series = moments[kind]
            cache[key] = 0.5 * (series[high + low] + series[high - low])
        return cache[key]

    solution_coords = {}
    one = jnp.ones_like(moments[("p", "p")][0])
    direction_coords = {("p", 0): one}
    residual_coords = {("r", 0): one}
    norm_now = bilinear(residual_coords, residual_coords, gram)
    for _ in range(STEPS):
        mapped = apply_shift(direction_coords)
        step_length = norm_now / bilinear(direction_coords, mapped, gram)
        solution_coords = plus(solution_coords, scaled(step_length, direction_coords))
        residual_coords = plus(residual_coords, scaled(-step_length, mapped))
        norm_next = bilinear(residual_coords, residual_coords, gram)
        direction_coords = plus(
            residual_coords, scaled(norm_next / norm_now, direction_coords)
        )
        norm_now = norm_next
    return solution_coords, residual_coords


def fold_sublanes(parts):
    row = lax.broadcasted_iota(jnp.int32, parts[0].shape, 0)
    parts = list(parts)
    span = 4
    while span:
        low = (row & span) == 0
        half = len(parts) // 2
        parts = [
            jnp.where(low, first, second)
            + pltpu.roll(jnp.where(low, second, first), span, 0)
            if span == 4
            else jnp.where(low, first, second)
            + jnp.where(low, pltpu.roll(first, 8 - span, 0), pltpu.roll(second, span, 0))
            for first, second in zip(parts[:half], parts[half:])
        ]
        span //= 2
    return parts[0]


def kernel(
    n_lat, n_lon, forcing_hbm, search_hbm, depth_hbm, mask_hbm, fold_hbm,
    out_height, out_residual, forcing, search, depth_in, mask_in, fold_map,
    depth, depth_e, depth_w, root, root_e, root_w, weights, basis, basis_halo,
    row_north, row_south, fold_rows, packed, got_north, got_south, got_east, got_west,
    corners, fold_all, dots, sums_lat, sums_lon, sums_all, moment_rows, load_sem,
    near_send, near_recv, fold_send, fold_recv, lat_send, lat_recv, lon_send, lon_recv,
    all_send, all_recv,
):
    rows, width = forcing_hbm.shape
    lat, lon = lax.axis_index("lat"), lax.axis_index("lon")
    top = n_lat - 1
    north, south = lax.rem(lat + 1, n_lat), lax.rem(lat + n_lat - 1, n_lat)
    east, west = lax.rem(lon + 1, n_lon), lax.rem(lon + n_lon - 1, n_lon)
    has_north, has_south = lat < top, lat > 0
    group_rows = rows * GROUP // width
    n_groups = width // GROUP

    barrier = pltpu.get_barrier_semaphore()

    def greet(place):
        pl.semaphore_signal(barrier, inc=1, device_id=place, device_id_type=MESH)

    loads = [
        pltpu.make_async_copy(source, target, load_sem.at[index])
        for index, (source, target) in enumerate(
            ((mask_hbm, mask_in), (depth_hbm, depth_in), (search_hbm, search),
             (forcing_hbm, forcing), (fold_hbm, fold_map))
        )
    ]
    for load in loads:
        load.start()
    direct = n_lat * n_lon <= DIRECT_LIMIT
    everyone = [(a, b) for a in range(n_lat) for b in range(n_lon) if a or b]
    everyone.sort(key=lambda d: -min(d[0], n_lat - d[0]) - min(d[1], n_lon - d[1]))
    if direct:
        for a, b in everyone:
            greet((lax.rem(lat + a, n_lat), lax.rem(lon + b, n_lon)))
        greeted = len(everyone)
    else:
        for d in range(1, n_lat):
            greet((lax.rem(lat + d, n_lat), lon))
        for d in range(1, n_lon):
            greet((lat, lax.rem(lon + d, n_lon)))
        for place in ((north, east), (north, west), (south, east), (south, west)):
            greet(place)
        greeted = n_lat - 1 + n_lon - 1 + 4

    for load in loads:
        load.wait()
    lane_group = lax.broadcasted_iota(jnp.int32, (group_rows, width), 1)
    west_edge = east_edge = None
    for g in range(n_groups):
        here = pl.ds(g * group_rows, group_rows)
        there = pl.ds(PAD + g * group_rows, group_rows)
        flag = mask_in[here, :].astype(jnp.float32)
        deep = depth_in[here, :] * flag
        moving = search[here, :] * flag
        left = forcing[here, :] * flag
        depth[0, there, :] = deep
        basis[0, there, :] = moving
        basis[STEPS + 1, there, :] = left
        inside = lane_group - g * GROUP
        to_west = jnp.where(
            inside < 9,
            turned(deep, g * GROUP),
            jnp.where(inside < 17, turned(moving, g * GROUP + 9), turned(left, g * GROUP + 17)),
        )
        to_east = jnp.where(
            inside < 9,
            turned(deep, g * GROUP + 9),
            jnp.where(inside < 17, turned(moving, g * GROUP + 17), turned(left, g * GROUP + 25)),
        )
        west_edge = to_west if g == 0 else jnp.where(inside >= 0, to_west, west_edge)
        east_edge = to_east if g == 0 else jnp.where(inside >= 0, to_east, east_edge)
    packed[0] = west_edge
    packed[1] = east_edge
    first, last = PAD, PAD + rows
    row_south[0:16, :] = depth[0, first : first + 16, :]
    row_south[16:24, :] = basis[0, first : first + 8, :]
    row_south[24:32, :] = basis[STEPS + 1, first : first + 8, :]
    row_north[0:16, :] = depth[0, last - 16 : last, :]
    row_north[16:24, :] = basis[0, last - 8 : last, :]
    row_north[24:32, :] = basis[STEPS + 1, last - 8 : last, :]

    @pl.when(lat == top)
    def _():
        for r in range(16):
            fold_rows[r : r + 1, :] = depth[0, last - 1 - r : last - r, :]
        for r in range(8):
            fold_rows[16 + r : 17 + r, :] = basis[0, last - 1 - r : last - r, :]
            fold_rows[24 + r : 25 + r, :] = basis[STEPS + 1, last - 1 - r : last - r, :]
        fold_all[lon] = fold_rows[...]

    pl.semaphore_wait(barrier, greeted)

    def near(index, source, target, place):
        return pltpu.make_async_remote_copy(
            src_ref=source, dst_ref=target, send_sem=near_send.at[index],
            recv_sem=near_recv.at[index], device_id=place, device_id_type=MESH,
        )

    tail = pl.ds(group_rows - 16, 16)
    head = pl.ds(0, 16)
    to_north = near(0, row_north, got_south, (north, lon))
    to_south = near(1, row_south, got_north, (south, lon))
    to_east = near(2, packed.at[1], got_west, (lat, east))
    to_west = near(3, packed.at[0], got_east, (lat, west))
    to_ne = near(4, packed.at[1, tail], corners.at[0], (north, east))
    to_nw = near(5, packed.at[0, tail], corners.at[1], (north, west))
    to_se = near(6, packed.at[1, head], corners.at[2], (south, east))
    to_sw = near(7, packed.at[0, head], corners.at[3], (south, west))
    northward, southward = (to_north, to_ne, to_nw), (to_south, to_se, to_sw)

    def spread(source, slots, send_sem, recv_sem, along_lat):
        size = n_lat if along_lat else n_lon
        me = lat if along_lat else lon
        copies = []
        for d in range(1, size):
            peer = lax.rem(me + d, size)
            copies.append(
                pltpu.make_async_remote_copy(
                    src_ref=source, dst_ref=slots.at[me], send_sem=send_sem.at[d - 1],
                    recv_sem=recv_sem.at[d - 1],
                    device_id=(peer, lon) if along_lat else (lat, peer),
                    device_id_type=MESH,
                )
            )
        return copies

    across = spread(fold_rows, fold_all, fold_send, fold_recv, False)

    @pl.when(lat == top)
    def _():
        for copy in across:
            copy.start()

    to_east.start()
    to_west.start()

    @pl.when(has_north)
    def _():
        for copy in northward:
            copy.start()

    @pl.when(has_south)
    def _():
        for copy in southward:
            copy.start()

    def unpack(got_e, got_w, start, g, count):
        lane = lax.broadcasted_iota(jnp.int32, (count, width), 1)
        base = -g * GROUP
        spans = ((0, 9, depth.at[1]), (9, 8, basis_halo.at[0]), (17, 8, basis_halo.at[STEPS + 1]))
        for offset, cells, target in spans:
            from_east = turned(got_e, base - offset)
            from_west = turned(got_w, base - offset - cells)
            target[start : start + count, :] = jnp.where(
                lane < cells,
                from_east,
                jnp.where(lane >= width - cells, from_west, jnp.zeros_like(got_e)),
            )

    to_east.wait_recv()
    to_west.wait_recv()
    for g in range(n_groups):
        unpack(got_east[...], got_west[...], PAD + g * group_rows, g, group_rows)

    @pl.when(has_south)
    def _():
        for copy in northward:
            copy.wait_recv()
        depth[0, 0:16, :] = got_south[0:16, :]
        basis[0, 8:16, :] = got_south[16:24, :]
        basis[STEPS + 1, 8:16, :] = got_south[24:32, :]
        unpack(corners[1], corners[0], 0, n_groups - 1, 16)

    @pl.when(lat == 0)
    def _():
        nothing = jnp.zeros((16, width), jnp.float32)
        for target in (depth.at[0], depth.at[1]):
            target[0:16, :] = nothing
        for power in (0, STEPS + 1):
            basis[power, 0:16, :] = nothing
            basis_halo[power, 0:16, :] = nothing

    @pl.when(has_north)
    def _():
        for copy in southward:
            copy.wait_recv()
        depth[0, last : last + 16, :] = got_north[0:16, :]
        basis[0, last : last + 8, :] = got_north[16:24, :]
        basis[STEPS + 1, last : last + 8, :] = got_north[24:32, :]
        unpack(corners[3], corners[2], last, 0, 16)

    @pl.when(lat == top)
    def _():
        for copy in across:
            copy.wait_recv()
        total = n_lon * width
        pivot = lax.rem(fold_map[0] - lon * width + total, total)
        block, offset = pivot // width, lax.rem(pivot, width)
        lane = lax.broadcasted_iota(jnp.int32, (32, width), 1)
        index = lax.rem(offset - lane + width, width)

        def mirrored(which):
            rows_of = fold_all[lax.rem(block + which + n_lon, n_lon)]
            return jnp.take_along_axis(rows_of, index, axis=1, mode="promise_in_bounds")

        ahead, same, behind, beyond = (mirrored(which) for which in (1, 0, -1, -2))
        close = lane <= offset
        centre = jnp.where(close, same, behind)
        halo = jnp.where(
            lane < width // 2, jnp.where(close, behind, beyond), jnp.where(close, ahead, same)
        )
        for value, deep, fields in ((centre, depth.at[0], basis), (halo, depth.at[1], basis_halo)):
            deep[last : last + 16, :] = value[0:16, :]
            fields[0, last : last + 8, :] = value[16:24, :]
            fields[STEPS + 1, last : last + 8, :] = value[24:32, :]

    low, high = PAD - 8, last + 8
    for at, count in chunks_of(0, rows + 2 * PAD, CHUNK):
        span = pl.ds(at, count)
        centre, halo = depth[0, span, :], depth[1, span, :]
        depth_e[0, span, :], depth_e[1, span, :] = shift_pair(centre, halo, 1)
        depth_w[0, span, :], depth_w[1, span, :] = shift_pair(centre, halo, -1)
    shifted_depth = {0: depth, 1: depth_e, -1: depth_w}
    for at, count in chunks_of(low, high, CHUNK):
        roots = []
        for tile in (0, 1):
            here = depth[tile, at : at + count, :]
            sums = {0.5: None, 0.25: None}
            for a, b in DIRECTIONS:
                beside = shifted_depth[b][tile, at + a : at + a + count, :]
                link = jnp.where(beside > 0.0, here + beside, 0.0)
                factor = halves((a, b))
                sums[factor] = link if sums[factor] is None else sums[factor] + link
            diagonal = here * (1.0 / (REACH * REACH)) + (0.5 * sums[0.5] + 0.25 * sums[0.25])
            value = lax.rsqrt(jnp.where(here > 0.0, diagonal, 1.0))
            root[tile, at : at + count, :] = value
            roots.append(value)
        span = pl.ds(at, count)
        root_e[0, span, :], root_e[1, span, :] = shift_pair(roots[0], roots[1], 1)
        root_w[0, span, :], root_w[1, span, :] = shift_pair(roots[0], roots[1], -1)
    shifted_root = {0: root, 1: root_e, -1: root_w}
    for at, count in chunks_of(low, high, CHUNK):
        for tile in (0, 1):
            for b in (-1, 0, 1):
                goal_depth = shifted_depth[-b][tile, at : at + count, :]
                goal_root = shifted_root[-b][tile, at : at + count, :]
                goal_wet = goal_depth > 0.0
                for a in (-1, 0, 1):
                    if (a, b) == (0, 0):
                        continue
                    from_depth = depth[tile, at + a : at + a + count, :]
                    from_root = root[tile, at + a : at + a + count, :]
                    link = jnp.where(
                        jnp.minimum(goal_depth, from_depth) > 0.0, goal_depth + from_depth, 0.0
                    )
                    weights[SLOT[(a, b)], tile, at : at + count, :] = (
                        goal_root * (-2.0 * halves((a, b)))
                    ) * (link * from_root)

    dot_sums = {}

    def add_dot(key, left, right):
        product = left * right
        for r in range(0, product.shape[0], 8):
            piece = product[r : r + 8, :]
            dot_sums[key] = piece if key not in dot_sums else dot_sums[key] + piece

    row_chunks = [(low, 8)] + chunks_of(first, last, CHUNK) + [(last, 8)]
    for at, count in chunks_of(first, last, CHUNK):
        p0 = basis[0, at : at + count, :]
        r0 = basis[STEPS + 1, at : at + count, :]
        add_dot(("p", "p", 0), p0, p0)
        add_dot(("r", "r", 0), r0, r0)
        add_dot(("p", "r", 0), p0, r0)

    for power in range(1, STEPS + 1):
        chains = [("p", 0, power == STEPS)]
        if power < STEPS:
            chains.append(("r", STEPS + 1, power == STEPS - 1))
        for at, count in row_chunks:
            inner = first <= at < last
            fresh = {}
            held = {}
            factors = [
                {ab: weights[SLOT[ab], tile, at : at + count, :] for ab in DIRECTIONS}
                for tile in (0, 1)
            ]
            for name, origin, only_block in chains:
                if only_block and not inner:
                    continue
                slot = origin + power
                parts = []
                for tile, fields in ((0, basis), (1, basis_halo)):
                    taken = {
                        a: fields[slot - 1, at + a : at + a + count, :] for a in (-1, 0, 1)
                    }
                    if tile == 0:
                        held[name] = taken[0]
                    columns = {}
                    for b in (-1, 0, 1):
                        total = None
                        for a in (-1, 0, 1):
                            if (a, b) == (0, 0):
                                continue
                            term = factors[tile][(a, b)] * taken[a]
                            total = term if total is None else total + term
                        columns[b] = total
                    parts.append(columns)
                ahead = shift_pair(parts[0][1], parts[1][1], 1)
                behind = shift_pair(parts[0][-1], parts[1][-1], -1)
                for tile, fields in ((0, basis), (1, basis_halo)):
                    if tile == 1 and only_block:
                        continue
                    value = parts[tile][0] + ahead[tile] + behind[tile]
                    if power == 1:
                        value = 0.5 * value
                    else:
                        value = value - fields[slot - 2, at : at + count, :]
                    fields[slot, at : at + count, :] = value
                    if tile == 0:
                        fresh[name] = value
            if not inner:
                continue
            for name, _, _ in chains:
                add_dot((name, name, 2 * power), fresh[name], fresh[name])
                add_dot((name, name, 2 * power - 1), fresh[name], held[name])
            if power < STEPS:
                add_dot(("p", "r", 2 * power), fresh["p"], fresh["r"])
                add_dot(("p", "r", 2 * power - 1), fresh["p"], held["r"])
            else:
                add_dot(
                    ("p", "r", 2 * power - 1),
                    fresh["p"],
                    basis[STEPS + power, at : at + count, :],
                )
        for key in [key for key in dot_sums]:
            dots[order_of()[key]] = dot_sums.pop(key)

    number = len(order_of())
    pending = []
    lane = lax.broadcasted_iota(jnp.int32, (8, width), 1)
    home = lane - lax.broadcasted_iota(jnp.int32, (8, width), 0)
    message = jnp.zeros((8, width), jnp.float32)
    for g in range(number // 8):
        grouped = fold_sublanes([dots[8 * g + s] for s in range(8)])
        message = jnp.where(home == 8 * g, jnp.sum(grouped, axis=1, keepdims=True), message)
    message = jnp.sum(message, axis=0, keepdims=True)
    if direct:
        me = lat * n_lon + lon
        sums_all[me] = message
        copies = [
            pltpu.make_async_remote_copy(
                src_ref=sums_all.at[me], dst_ref=sums_all.at[me], send_sem=all_send.at[index],
                recv_sem=all_recv.at[index],
                device_id=(lax.rem(lat + a, n_lat), lax.rem(lon + b, n_lon)),
                device_id_type=MESH,
            )
            for index, (a, b) in enumerate(everyone)
        ]
        rounds = ((sums_all, n_lat * n_lon, copies),)
    else:
        rounds = (
            (sums_lat, n_lat, None, lat, True, lat_send, lat_recv),
            (sums_lon, n_lon, None, lon, False, lon_send, lon_recv),
        )
    for slots, size, copies, *rest in rounds:
        if copies is None:
            me, along_lat, send_sem, recv_sem = rest
            slots[me] = message
            copies = spread(slots.at[me], slots, send_sem, recv_sem, along_lat)
        for copy in copies:
            copy.start()
        for copy in copies:
            copy.wait_recv()
        terms = [slots[index] for index in range(size)]
        while len(terms) > 1:
            odd = terms[len(terms) // 2 * 2 :]
            terms = [x + y for x, y in zip(terms[0::2], terms[1::2])] + odd
        message = terms[0]
        pending.extend(copies)
    message = jnp.broadcast_to(message, (8, width))
    for g in range(number // 8):
        picked = jnp.sum(jnp.where(home == 8 * g, message, 0.0), axis=1, keepdims=True)
        moment_rows[8 * g : 8 * g + 8, :] = jnp.broadcast_to(picked, (8, width))
    moments = {}
    for kind in (("p", "p"), ("p", "r"), ("r", "r")):
        series = []
        for index in range(17 if kind == ("p", "p") else 16 if kind == ("p", "r") else 15):
            spot = order_of()[kind + (index,)]
            value = jnp.broadcast_to(moment_rows[spot : spot + 1, :], (8, width))
            series.append(value if index < 2 else 2.0 * value - series[index % 2])
        moments[kind] = series
    height_coords, residual_coords = coordinates(moments)
    for at in range(0, rows, 8):
        for coords, out in ((height_coords, out_height), (residual_coords, out_residual)):
            total = None
            for (chain, power), factor in sorted(coords.items(), key=lambda item: item[0]):
                slot = power + (0 if chain == "p" else STEPS + 1)
                term = factor * basis[slot, PAD + at : PAD + at + 8, :]
                total = term if total is None else total + term
            out[at : at + 8, :] = total

    for copy in pending:
        copy.wait_send()
    to_east.wait_send()
    to_west.wait_send()

    @pl.when(has_north)
    def _():
        for copy in northward:
            copy.wait_send()

    @pl.when(has_south)
    def _():
        for copy in southward:
            copy.wait_send()

    @pl.when(lat == top)
    def _():
        for copy in across:
            copy.wait_send()


@functools.cache
def order_of():
    keys = [("p", "p", k) for k in range(2 * STEPS + 1)]
    keys += [("p", "r", k) for k in range(2 * STEPS)]
    keys += [("r", "r", k) for k in range(2 * STEPS - 1)]
    return {key: index for index, key in enumerate(keys)}


def hand_over(height, residual, out_height, out_residual):
    out_height[...] = height[...]
    out_residual[...] = residual[...]


def per_device(n_lat, n_lon, forcing, search_direction, ocean_depth, land_mask, fold_map):
    rows, width = forcing.shape
    tall = rows + 2 * PAD
    f32 = jnp.float32
    own = pltpu.VMEM((rows, width), f32)
    pair = pltpu.VMEM((2, tall, width), f32)
    edge = pltpu.VMEM((32, width), f32)
    group_rows = rows * GROUP // width
    strip = pltpu.VMEM((group_rows, width), f32)
    everyone = n_lat * n_lon if n_lat * n_lon <= DIRECT_LIMIT else 2
    dma = pltpu.SemaphoreType.DMA
    block = pl.BlockSpec(memory_space=pltpu.VMEM)
    outs = pl.pallas_call(
        functools.partial(kernel, n_lat, n_lon),
        out_shape=[jax.ShapeDtypeStruct((rows, width), f32)] * 2,
        in_specs=[pl.BlockSpec(memory_space=pl.ANY)] * 5,
        out_specs=[block] * 2,
        scratch_shapes=[
            own, own, own, pltpu.VMEM((rows, width), jnp.int32),
            pltpu.SMEM(fold_map.shape, jnp.int32),
            pair, pair, pair, pair, pair, pair,
            pltpu.VMEM((8, 2, tall, width), f32),
            pltpu.VMEM((2 * STEPS + 1, tall, width), f32),
            pltpu.VMEM((2 * STEPS + 1, tall, width), f32),
            edge, edge, edge,
            pltpu.VMEM((2, group_rows, width), f32),
            edge, edge, strip, strip,
            pltpu.VMEM((4, 16, width), f32),
            pltpu.VMEM((n_lon, 32, width), f32),
            pltpu.VMEM((6 * STEPS, 8, width), f32),
            pltpu.VMEM((n_lat, 1, width), f32),
            pltpu.VMEM((n_lon, 1, width), f32),
            pltpu.VMEM((everyone, 1, width), f32),
            pltpu.VMEM((6 * STEPS, width), f32),
            dma((5,)),
            dma((8,)), dma((8,)),
            dma((n_lon - 1,)), dma((n_lon - 1,)),
            dma((n_lat - 1,)), dma((n_lat - 1,)),
            dma((n_lon - 1,)), dma((n_lon - 1,)),
            dma((everyone - 1,)), dma((everyone - 1,)),
        ],
        compiler_params=pltpu.CompilerParams(collective_id=0, has_side_effects=True),
        name="tripole_cg",
    )(forcing, search_direction, ocean_depth, land_mask, fold_map)
    return pl.pallas_call(
        hand_over,
        out_shape=[jax.ShapeDtypeStruct((rows, width), f32)] * 2,
        in_specs=[block] * 2,
        out_specs=[block] * 2,
        name="hand_over",
    )(*outs)


def solution(mesh):
    cells = P("lat", "lon")
    return jax.shard_map(
        functools.partial(per_device, mesh.shape["lat"], mesh.shape["lon"]),
        mesh=mesh,
        in_specs=(cells, cells, cells, cells, P()),
        out_specs=(cells, cells),
        check_vma=False,
    )
```
